32 devices in a mesh: parts: 2 (over y), rows: 4 (over z), cols: 2 (over x), rank: 2 (over core).
Axes of the slice: x: 2, y: 2, z: 4, core: 2. Of those that a mesh axis runs over, the one named last changes fastest.
Arguments:
- probes: bfloat16 [32768, 128], P(('parts', 'rows', 'cols')), parts along dimension 0, may hold values from -6 to 6
- basis_one: bfloat16 [32768, 256], P(('parts', 'rows', 'cols'), 'rank'), parts along dimension 0, may hold values from -0.375 to 0.375
- basis_two: bfloat16 [32768, 256], P(('parts', 'rows', 'cols'), 'rank'), parts along dimension 0, may hold values from -0.375 to 0.375
- basis_three: bfloat16 [32768, 256], P(('parts', 'rows', 'cols'), 'rank'), parts along dimension 0, may hold values from -0.375 to 0.375
- coeff_one: bfloat16 [32768, 256], P(('parts', 'rows', 'cols'), 'rank'), parts along dimension 0, may hold values from -0.0625 to 0.0625
- coeff_two: bfloat16 [32768, 256], P(('parts', 'rows', 'cols'), 'rank'), parts along dimension 0, may hold values from -0.09375 to 0.09375
- coeff_three: bfloat16 [32768, 256], P(('parts', 'rows', 'cols'), 'rank'), parts along dimension 0, may hold values from -0.125 to 0.125
- leaves: bfloat16 [128, 256, 256], P(('parts', 'rows', 'cols', 'rank')), parts along dimension 0, may hold values from -0.375 to 0.375
Outputs:
- covariance_power: bfloat16 [32768, 128], P(('parts', 'rows', 'cols', 'rank')), parts along dimension 0
The draws below stay inside these ranges and needn't reach their ends.
There are 2 independent parts, one for each index of `parts`. The reference program is written for one: setup_inputs(seed, part) draws one part's arguments, and reference() takes and returns one part's arrays. A program takes and returns all parts, laid end to end along the dimension named above; each array names one. Nothing has to cross between parts.
All inputs are finite; a program needn't handle non-finite values.
Results may differ from the reference program's by a relative error of at most 0.017.
Values may be sent and summed in bfloat16 or wider, within the bound.
A program may use at most 64 MiB of HBM per device.

```python
import jax
import jax.numpy as jnp
from jax import lax

K = 256
C = 128
LEAF = 256
PASSES = 2
NPTS = 16384


def block_scale(rng, dims, cuts, low, high):
    loudness = 1.0
    for dim, blocks in cuts:
        steps = jax.random.uniform(jax.random.fold_in(jax.random.fold_in(rng, 6), dim), (blocks,), jnp.float32, low / len(cuts), high / len(cuts))
        loudness = loudness * jnp.repeat(jnp.exp(steps), dims[dim] // blocks).reshape((-1,) + (1,) * (len(dims) - 1 - dim))
    return loudness


def scatter_about(key, dims, width, reach, split=(), kind=jnp.bfloat16):
    drawn = width * jax.random.normal(key, dims, jnp.float32)
    if split:
        drawn = drawn * block_scale(key, dims, split, -0.22, 0.18)
    return jnp.clip(drawn, -reach, reach).astype(kind)


def setup_inputs(seed: int = 0, part: int = 0) -> dict:
    keys = jax.random.split(jax.random.key(seed), 9)
    own_keys = jax.random.split(jax.random.fold_in(keys[8], part), 9)
    return {
        "probes": scatter_about(own_keys[0], (NPTS, C), 1.0, 6.0, ((0, 8),)),
        "basis_one": scatter_about(own_keys[1], (NPTS, K), K ** -0.5, 0.375, ((0, 8), (1, 2))),
        "basis_two": scatter_about(own_keys[2], (NPTS, K), K ** -0.5, 0.375, ((0, 8), (1, 2))),
        "basis_three": scatter_about(own_keys[3], (NPTS, K), K ** -0.5, 0.375, ((0, 8), (1, 2))),
        "coeff_one": scatter_about(own_keys[4], (NPTS, K), (NPTS // 2) ** -0.5, 0.0625, ((0, 8), (1, 2))),
        "coeff_two": scatter_about(own_keys[5], (NPTS, K), (NPTS // 4) ** -0.5, 0.09375, ((0, 8), (1, 2))),
        "coeff_three": scatter_about(own_keys[6], (NPTS, K), (NPTS // 8) ** -0.5, 0.125, ((0, 8), (1, 2))),
        "leaves": scatter_about(own_keys[7], (NPTS // LEAF, LEAF, LEAF), LEAF ** -0.5, 0.375, ((0, 16),)),
    }


def apply_once(current, outside, inside, leaves, flipped):
    values = current.astype(jnp.float32)
    summed = jnp.zeros((NPTS, C), jnp.float32)
    for level_index in range(3):
        blocks = 2 ** (level_index + 1)
        former = inside[level_index].astype(jnp.float32).reshape(blocks, -1, K)
        pieces = values.reshape(blocks, -1, C)
        projected = jnp.einsum("bnk,bnc->bkc", former, pieces, precision=lax.Precision.HIGHEST).astype(jnp.bfloat16)
        swapped = projected.reshape(blocks // 2, 2, K, C)[:, ::-1].reshape(blocks, K, C).astype(jnp.float32)
        latter = outside[level_index].astype(jnp.float32).reshape(blocks, -1, K)
        summed = summed + jnp.einsum("bnk,bkc->bnc", latter, swapped, precision=lax.Precision.HIGHEST).reshape(NPTS, C)
    dense = leaves.astype(jnp.float32)
    pieces = values.reshape(-1, LEAF, C)
    pattern = "bji,bjc->bic" if flipped else "bij,bjc->bic"
    summed = summed + jnp.einsum(pattern, dense, pieces, precision=lax.Precision.HIGHEST).reshape(NPTS, C)
    return summed.astype(jnp.bfloat16)


def reference(probes, basis_one, basis_two, basis_three, coeff_one, coeff_two, coeff_three, leaves):
    uppers = (basis_one, basis_two, basis_three)
    lowers = (coeff_one, coeff_two, coeff_three)
    current = probes
    for repeat in range(PASSES):
        current = apply_once(current, lowers, uppers, leaves, True)
        current = apply_once(current, uppers, lowers, leaves, False)
    return current
```

```python
import functools

import jax
import jax.numpy as jnp
from jax import lax
from jax.experimental import pallas as pl
from jax.experimental.pallas import tpu as pltpu
from jax.sharding import PartitionSpec as P

PASSES = 2
LEVELS = 3
MESH = pl.DeviceIdType.MESH
F32 = jnp.float32


def flip(value, mask):
    bit = 1
    out = value
    while bit <= mask:
        if mask & bit:
            out = out + (1 - 2 * lax.rem(lax.div(value, jnp.int32(bit)), jnp.int32(2))) * bit
        bit *= 2
    return out


def make_stages(bits):
    stages = []
    for level in range(1, LEVELS + 1):
        reduce_bits = bits - level
        rounds = []
        bit = 0
        while bit < reduce_bits:
            if bit + 1 < reduce_bits:
                rounds.append([1 << bit, 2 << bit, 3 << bit])
                bit += 2
            else:
                rounds.append([1 << bit])
                bit += 1
        rounds.append([1 << reduce_bits])
        stages.append(rounds)
    return stages


def tdot(a, b):
    return lax.dot_general(a, b, (((0,), (0,)), ((), ())), preferred_element_type=F32)


def dot(a, b):
    return jnp.dot(a, b, preferred_element_type=F32)


def kernel(stages, cols_n, probes, b1, b2, b3, c1, c2, c3, leaves, out,
           fac, far, z_own, z_far, lv, acc, proj, rbuf, sbuf, lsem, fss, frs, ss, rs):
    uppers, lowers = (b1, b2, b3), (c1, c2, c3)
    half = z_own.shape[0]
    leaf = leaves.shape[1]
    part = lax.axis_index("parts")
    position = lax.axis_index("rows") * cols_n + lax.axis_index("cols")
    rank = lax.axis_index("rank")

    def peer(mask):
        other = flip(position, mask)
        return (part, lax.div(other, jnp.int32(cols_n)), lax.rem(other, jnp.int32(cols_n)), rank)

    twin = (part, lax.axis_index("rows"), lax.axis_index("cols"), 1 - rank)
    masks = sorted({m for rounds in stages for masks in rounds for m in masks})
    peers = {m: peer(m) for m in masks}

    barrier = pltpu.get_barrier_semaphore()
    for device in [twin] + list(peers.values()):
        pl.semaphore_signal(barrier, inc=1, device_id=device, device_id_type=MESH)

    own_rows = pl.ds(pl.multiple_of(rank * half, half), half)
    far_rows = pl.ds(pl.multiple_of((1 - rank) * half, half), half)
    loads = []

    def load(src, dst):
        copy = pltpu.make_async_copy(src, dst, lsem.at[len(loads)])
        copy.start()
        loads.append(copy)
        return copy

    load_z = [load(probes.at[own_rows], z_own), load(probes.at[far_rows], z_far)]
    load_up = [
        (load(uppers[i].at[own_rows], fac.at[i, 0]), load(uppers[i].at[far_rows], far.at[i]))
        for i in range(LEVELS)
    ]
    load_leaves = load(leaves, lv)
    load_low = [load(lowers[i].at[own_rows], fac.at[LEVELS + i, 0]) for i in range(LEVELS)]

    for copy in load_z:
        copy.wait()
    started = []
    counts = {"r": 0, "s": 0}

    def send(src, device):
        slot = counts["r"]
        counts["r"] += 1
        copy = pltpu.make_async_remote_copy(
            src_ref=src, dst_ref=rbuf.at[slot], send_sem=ss.at[slot], recv_sem=rs.at[slot],
            device_id=device, device_id_type=MESH)
        copy.start()
        started.append(copy)
        return copy, slot

    def stage_out(value):
        slot = counts["s"]
        counts["s"] += 1
        sbuf[slot] = value.astype(sbuf.dtype)
        return sbuf.at[slot]

    trade = [None] * (2 * LEVELS)
    applies = 2 * PASSES
    total_rounds = max(len(rounds) for rounds in stages)
    for step in range(applies):
        flipped = step % 2 == 0
        inside = 0 if flipped else LEVELS
        outside = LEVELS if flipped else 0
        twin_part = [None] * LEVELS
        if step == 0:
            for i in range(LEVELS):
                for copy in load_up[i]:
                    copy.wait()
                proj[i] = tdot(fac[i, 0], z_own[...]) + tdot(far[i], z_far[...])
            pl.semaphore_wait(barrier, 1 + len(masks))
        else:
            z = z_own[...]
            for i in range(LEVELS):
                twin_part[i] = send(stage_out(tdot(fac[inside + i, 1], z)), twin)
            for i in range(LEVELS):
                proj[i] = tdot(fac[inside + i, 0], z)

        in_flight = [None] * LEVELS
        finals = []

        def own_term(i, slot, outside=outside):
            if step == 0:
                load_low[i].wait()
            acc[...] += dot(fac[outside + i, 0], rbuf[slot])

        def twin_term(i, copy, slot, outside=outside):
            if step <= 1:
                trade[outside + i].wait_recv()
            copy.wait_recv()
            acc[...] += dot(fac[outside + i, 1], rbuf[slot])

        for turn in range(total_rounds + 1):
            order = range(LEVELS) if turn < total_rounds else reversed(range(LEVELS))
            for i in order:
                rounds = stages[i]
                if turn == 0:
                    if twin_part[i] is not None:
                        copy, slot = twin_part[i]
                        copy.wait_recv()
                        proj[i] += rbuf[slot].astype(F32)
                elif turn <= len(rounds):
                    for copy, _ in in_flight[i]:
                        copy.wait_recv()
                    if turn < len(rounds):
                        total = proj[i]
                        for _, slot in in_flight[i]:
                            total = total + rbuf[slot].astype(F32)
                        proj[i] = total
                    else:
                        _, slot = in_flight[i][0]
                        forward = send(rbuf.at[slot], twin)
                        own_term(i, slot)
                        for item in finals:
                            twin_term(*item)
                        finals = [(i,) + forward]
                if turn < len(rounds):
                    source = stage_out(proj[i])
                    in_flight[i] = [send(source, peers[m]) for m in rounds[turn]]
            if turn == 0:
                if step == 0:
                    for i in range(2 * LEVELS):
                        k = (i + LEVELS) % (2 * LEVELS)
                        src = far.at[k] if k < LEVELS else lowers[k - LEVELS].at[far_rows]
                        trade[k] = pltpu.make_async_remote_copy(
                            src_ref=src, dst_ref=fac.at[k, 1], send_sem=fss.at[k], recv_sem=frs.at[k],
                            device_id=twin, device_id_type=MESH)
                        trade[k].start()
                        started.append(trade[k])
                    load_leaves.wait()
                for q in range(half // leaf):
                    rows = slice(q * leaf, (q + 1) * leaf)
                    piece = z_own[rows]
                    acc[rows] = tdot(lv[q], piece) if flipped else dot(lv[q], piece)
        for item in finals:
            twin_term(*item)
        if step + 1 < applies:
            z_own[...] = acc[...].astype(z_own.dtype)
        else:
            out[...] = acc[...].astype(out.dtype)
    for copy in started:
        copy.wait_send()


def local(mesh, probes, *rest):
    rows_n, cols_n = mesh.shape["rows"], mesh.shape["cols"]
    stages = make_stages((rows_n * cols_n).bit_length() - 1)
    factor, leaves = rest[0], rest[-1]
    half = probes.shape[0] // mesh.shape["rank"]
    c = probes.shape[1]
    k = factor.shape[1]
    applies = 2 * PASSES
    n_recv = applies * (sum(len(m) for rounds in stages for m in rounds) + LEVELS) + (applies - 1) * LEVELS
    n_send = applies * sum(len(rounds) for rounds in stages) + (applies - 1) * LEVELS
    bf16 = probes.dtype
    return pl.pallas_call(
        functools.partial(kernel, stages, cols_n),
        out_shape=jax.ShapeDtypeStruct((half, c), bf16),
        in_specs=[pl.BlockSpec(memory_space=pl.ANY)] * (2 + 2 * LEVELS),
        out_specs=pl.BlockSpec(memory_space=pltpu.VMEM),
        scratch_shapes=[
            pltpu.VMEM((2 * LEVELS, 2, half, k), bf16),
            pltpu.VMEM((LEVELS, half, k), bf16),
            pltpu.VMEM((half, c), bf16),
            pltpu.VMEM((half, c), bf16),
            pltpu.VMEM(leaves.shape, bf16),
            pltpu.VMEM((half, c), F32),
            pltpu.VMEM((LEVELS, k, c), F32),
            pltpu.VMEM((n_recv, k, c), bf16),
            pltpu.VMEM((n_send, k, c), bf16),
            pltpu.SemaphoreType.DMA((3 + 3 * LEVELS,)),
            pltpu.SemaphoreType.DMA((2 * LEVELS,)),
            pltpu.SemaphoreType.DMA((2 * LEVELS,)),
            pltpu.SemaphoreType.DMA((n_recv,)),
            pltpu.SemaphoreType.DMA((n_recv,)),
        ],
        compiler_params=pltpu.CompilerParams(collective_id=0, has_side_effects=True),
    )(probes, *rest)


def solution(mesh):
    rows = ("parts", "rows", "cols")
    in_specs = (P(rows, None),) + (P(rows, "rank"),) * (2 * LEVELS) + (P(rows + ("rank",), None, None),)
    out_specs = P(rows + ("rank",), None)
    return jax.shard_map(
        functools.partial(local, mesh), mesh=mesh, in_specs=in_specs, out_specs=out_specs, check_vma=False)
```
